32 devices in a mesh: groups: 2 (over y), space: 4 (over z), rhs: 4 (over x, core).
Axes of the slice: x: 2, y: 2, z: 4, core: 2. Of those that a mesh axis runs over, the one named last changes fastest.
Arguments:
- conductance: float32 [64, 1024], P(('groups', 'space')), parts along dimension 0, may hold values from 0.05 to 2
- nodata: int32 [64, 1024], P(('groups', 'space')), parts along dimension 0, may hold values 0 or 1
- ground_mask: int32 [64, 1024], P(('groups', 'space')), parts along dimension 0, may hold values 0 or 1
- ground_value: float32 [64, 1024], P(('groups', 'space')), parts along dimension 0, may hold values from 0.5 to 4
- source_mask: int32 [64, 1024], P(('groups', 'space')), parts along dimension 0, may hold values 0 or 1
- source_current: float32 [64, 1024], P(('groups', 'space')), parts along dimension 0, may hold values from 0.5 to 4
- tile_inverse: float32 [64, 8, 128, 128], P(('groups', 'space')), parts along dimension 0, may hold values from -0.04 to 8, as said below
- focal_cells: int32 [512, 2], P(('groups', 'rhs')), parts along dimension 0, may hold values from 0 to 32767
Outputs:
- solution: float32 [256, 64, 1024], P('rhs', ('groups', 'space')), parts along dimension 1
- residual: float32 [256, 64, 1024], P('rhs', ('groups', 'space')), parts along dimension 1
The draws below stay inside these ranges and needn't reach their ends.
There are 2 independent parts, one for each index of `groups`. The reference program is written for one: setup_inputs(seed, part) draws one part's arguments, and reference() takes and returns one part's arrays. A program takes and returns all parts, laid end to end along the dimension named above; each array names one. Nothing has to cross between parts.
Inputs may be any that keep to these rules, and one draw needn't show every extreme that they name: `tile_inverse`: each block is symmetric positive definite.
All inputs are finite; a program needn't handle non-finite values. No bound on the sum of `nodata` or of `ground_mask` or of `source_mask` on one device may be relied on, other than what follows from the above.
Results may differ from the reference program's by a relative error of at most 0.00025.
Values sent between devices are 32-bit elements; how exact they have to be, the bound alone decides.
A program may use at most 64 MiB of HBM per device.

```python
import math
import jax
import jax.numpy as jnp
from jax import lax

NC = 1024
ITERS = 2
NR = 32
PAIRS = 256


def draw_tile_inverse(key, part):
    key_off, key_diag = jax.random.split(jax.random.fold_in(key, 7))
    block_shape = (NR, NC // 128, 128, 128)
    spread_top = 0.02
    lower_end = 0.5
    upper_end = 1.5
    raw_values = jax.random.uniform(key_off, block_shape, jnp.float32, -spread_top, spread_top)
    upper_half = jnp.triu(raw_values, 1)
    off_part = upper_half + jnp.swapaxes(upper_half, -1, -2)
    base_part = jax.random.uniform(key_diag, block_shape[:-1], jnp.float32, lower_end, upper_end)
    diag_part = jnp.sum(jnp.abs(off_part), axis=-1) + base_part
    return off_part + diag_part[..., None] * jnp.eye(128, dtype=jnp.float32)


def set_ends(values, rng, least, high):
    place = [jax.random.randint(jax.random.fold_in(rng, axis), (), 0, length) for axis, length in enumerate(values.shape)]
    main_axis = values.shape.index(max(values.shape))
    neighbour = place[:main_axis] + [(place[main_axis] + 1) % values.shape[main_axis]] + place[main_axis + 1:]
    return values.at[tuple(place)].set(least).at[tuple(neighbour)].set(high)


def shard_levels(key, shape, cuts, smallest, top_value):
    gain, own = 1.0, jax.random.fold_in(key, 6)
    for dim, blocks in cuts:
        heights = jnp.exp(jax.random.uniform(jax.random.fold_in(own, dim), (blocks,), jnp.float32, smallest / len(cuts), top_value / len(cuts)))
        gain = gain * jnp.repeat(heights, shape[dim] // blocks).reshape([-1 if axis == dim else 1 for axis in range(len(shape))])
    return gain


def setup_inputs(seed: int = 0, part: int = 0) -> dict:
    keys = jax.random.split(jax.random.key(seed), 9)
    part_keys = jax.random.split(jax.random.fold_in(keys[8], part), 9)
    return {
        "conductance": jnp.clip(jnp.exp(math.log(2.0) - 3.6888794 * jax.random.uniform(part_keys[0], (NR, NC), jnp.float32) ** shard_levels(part_keys[0], (NR, NC), ((0, 4),), -0.2, 0.2)), 0.05, 2.0),
        "nodata": set_ends((jax.random.randint(part_keys[1], (NR, NC), 0, 10) < 1).astype(jnp.int32), jax.random.fold_in(part_keys[1], 1), 0, 1),
        "ground_mask": set_ends((jax.random.randint(part_keys[2], (NR, NC), 0, 20) < 1).astype(jnp.int32), jax.random.fold_in(part_keys[2], 1), 0, 1),
        "ground_value": jnp.clip(jnp.exp(math.log(4.0) - 2.0794415 * jax.random.uniform(part_keys[3], (NR, NC), jnp.float32) ** shard_levels(part_keys[3], (NR, NC), ((0, 4),), -0.2, 0.2)), 0.5, 4.0),
        "source_mask": set_ends((jax.random.randint(part_keys[4], (NR, NC), 0, 3) < 1).astype(jnp.int32), jax.random.fold_in(part_keys[4], 1), 0, 1),
        "source_current": jnp.clip(jnp.exp(math.log(4.0) - 2.0794415 * jax.random.uniform(part_keys[5], (NR, NC), jnp.float32) ** shard_levels(part_keys[5], (NR, NC), ((0, 4),), -0.2, 0.2)), 0.5, 4.0),
        "tile_inverse": draw_tile_inverse(jax.random.fold_in(jax.random.fold_in(keys[8], part), 71), part),
        "focal_cells": set_ends(jax.random.randint(part_keys[7], (PAIRS, 2), 0, NR * NC), jax.random.fold_in(part_keys[7], 1), 0, (NR * NC) - 1).astype(jnp.int32),
    }


LEAKAGE = 0.05
FOCAL_CURRENT = 16.0


def weights_from(padded_g, padded_v, valid_mask, ground_mask, ground_value):
    centre = padded_g[1:-1, 1:-1]
    north_w = 0.5 * (centre + padded_g[:-2, 1:-1]) * valid_mask * padded_v[:-2, 1:-1]
    south_w = 0.5 * (centre + padded_g[2:, 1:-1]) * valid_mask * padded_v[2:, 1:-1]
    west_w = 0.5 * (centre + padded_g[1:-1, :-2]) * valid_mask * padded_v[1:-1, :-2]
    east_w = 0.5 * (centre + padded_g[1:-1, 2:]) * valid_mask * padded_v[1:-1, 2:]
    grounded = ground_mask.astype(jnp.float32) * ground_value
    diagonal = valid_mask * (LEAKAGE + grounded) + (1.0 - valid_mask) + north_w + south_w + west_w + east_w
    return diagonal, north_w, south_w, west_w, east_w


def stencil(padded, weights):
    diagonal, north_w, south_w, west_w, east_w = weights
    centre = padded[:, 1:-1, 1:-1]
    return (diagonal * centre - north_w * padded[:, :-2, 1:-1] - south_w * padded[:, 2:, 1:-1]
            - west_w * padded[:, 1:-1, :-2] - east_w * padded[:, 1:-1, 2:])


def precondition(field_in, tile_inverse):
    pair_count, row_count, col_count = field_in.shape
    blocks = field_in.reshape(pair_count, row_count, col_count // 128, 128)
    result = jnp.einsum("rcij,prcj->prci", tile_inverse, blocks,
                        precision=lax.Precision.HIGHEST, preferred_element_type=jnp.float32)
    return result.reshape(pair_count, row_count, col_count)


def inner_sum(first, second):
    return jnp.sum(first * second, axis=(1, 2))


def reference(conductance, nodata, ground_mask, ground_value, source_mask, source_current, tile_inverse, focal_cells):
    valid_mask = (1 - nodata).astype(jnp.float32)
    active = conductance * valid_mask
    weights = weights_from(jnp.pad(active, 1), jnp.pad(valid_mask, 1), valid_mask, ground_mask, ground_value)
    row_count, col_count = conductance.shape
    cell_ids = jnp.arange(row_count * col_count, dtype=jnp.int32)
    onehot = ((cell_ids[None, :] == focal_cells[:, 0:1]).astype(jnp.float32)
              - (cell_ids[None, :] == focal_cells[:, 1:2]).astype(jnp.float32))
    onehot = onehot.reshape(focal_cells.shape[0], row_count, col_count)
    background = source_mask.astype(jnp.float32) * source_current
    right_side = background[None] + FOCAL_CURRENT * onehot
    solution = jnp.zeros_like(right_side)
    residual = right_side
    precond = precondition(residual, tile_inverse)
    direction = precond
    gamma_now = inner_sum(residual, precond)
    for iteration in range(ITERS):
        padded = jnp.pad(direction, ((0, 0), (1, 1), (1, 1)))
        image = stencil(padded, weights)
        step_len = gamma_now / inner_sum(direction, image)
        solution = solution + step_len[:, None, None] * direction
        residual = residual - step_len[:, None, None] * image
        if iteration + 1 < ITERS:
            precond = precondition(residual, tile_inverse)
            gamma_next = inner_sum(residual, precond)
            direction = precond + (gamma_next / gamma_now)[:, None, None] * direction
            gamma_now = gamma_next
    return solution, residual
```

```python
import functools

import jax
import jax.numpy as jnp
from jax import lax
from jax.experimental import pallas as pl
from jax.experimental.pallas import tpu as pltpu
from jax.sharding import PartitionSpec as P

LEAKAGE = 0.05
FOCAL_CURRENT = 16.0
LANES = 128
EXTRA = 8
F32 = jnp.float32
BF16 = jnp.bfloat16


def fold(x):
    out = x[:, :LANES]
    for c in range(1, x.shape[1] // LANES):
        out = out + x[:, c * LANES:(c + 1) * LANES]
    return out


def krylov_kernel(
    count, cond_ref, nodata_ref, gmask_ref, gval_ref, smask_ref, scur_ref, t_ref, focal_ref,
    q_ref, w_ref, z_ref, y_ref, coef_ref,
    r0_ref, thl_ref, wts_ref, qhalo_ref, zhalo_ref, msg_ref, got_ref, acc_ref, stat_ref, all_ref,
    send1, recv1, send2, recv2, send3, recv3,
):
    rows, cols = cond_ref.shape
    tiles = cols // LANES
    pairs = focal_ref.shape[0]
    ext = pairs + EXTRA
    groups = ext // 8
    me = lax.axis_index("space")
    last = count - 1

    barrier = pltpu.get_barrier_semaphore()
    for off in range(1, count):
        pl.semaphore_signal(
            barrier, inc=1, device_id={"space": lax.rem(me + off, count)},
            device_id_type=pl.DeviceIdType.MESH,
        )

    valid = (1 - nodata_ref[...]).astype(F32)
    active = cond_ref[...] * valid
    grounded = gmask_ref[...].astype(F32) * gval_ref[...]
    background = smask_ref[...].astype(F32) * scur_ref[...]

    def set_weights(up_a, up_v, down_a, down_v):
        lane = lax.broadcasted_iota(jnp.int32, (rows, cols), 1)
        zero = jnp.zeros((rows, cols), F32)
        row = lax.broadcasted_iota(jnp.int32, (rows, cols), 0)

        def edge(a, v):
            return 0.5 * (active + a) * valid * v

        def west(x):
            return jnp.where(lane == 0, zero, pltpu.roll(x, 1, 1))

        def east(x):
            return jnp.where(lane == cols - 1, zero, pltpu.roll(x, cols - 1, 1))

        def north(x, h):
            return jnp.where(row == 0, jnp.broadcast_to(h, x.shape), pltpu.roll(x, 1, 0))

        def south(x, h):
            return jnp.where(row == rows - 1, jnp.broadcast_to(h, x.shape), pltpu.roll(x, rows - 1, 0))

        nw = edge(north(active, up_a), north(valid, up_v))
        sw = edge(south(active, down_a), south(valid, down_v))
        ww = edge(west(active), west(valid))
        ew = edge(east(active), east(valid))
        dg = valid * (LEAKAGE + grounded) + (1.0 - valid) + nw + sw + ww + ew
        for r in range(rows):
            for i, x in enumerate((dg, nw, sw, ww, ew)):
                wts_ref[r, i:i + 1, :] = x[r:r + 1, :]

    none = jnp.zeros((1, cols), F32)
    set_weights(none, none, none, none)

    acc_ref[...] = jnp.zeros(acc_ref.shape, F32)
    fa = jnp.concatenate([focal_ref[:, 0:1], jnp.full((EXTRA, 1), -1, jnp.int32)], 0)
    fb = jnp.concatenate([focal_ref[:, 1:2], jnp.full((EXTRA, 1), -1, jnp.int32)], 0)

    for r in range(rows):
        ids = (me * rows + r) * cols + lax.broadcasted_iota(jnp.int32, (ext, cols), 1)
        onehot = (ids == fa).astype(F32) - (ids == fb).astype(F32)
        r0_ref[r] = background[r:r + 1, :] + FOCAL_CURRENT * onehot

    def precond_row(src, dst, r, split):
        for c in range(tiles):
            cut = slice(c * LANES, (c + 1) * LANES)
            if split:
                t = t_ref[r, c]
                thi = t.astype(BF16)
                thl_ref[r, c, :, :LANES] = thi
                thl_ref[r, c, :, LANES:] = (t - thi.astype(F32)).astype(BF16)
            x = src[r, :, cut]
            hi = x.astype(BF16).astype(F32)
            lhs = jnp.concatenate([hi, x - hi], 0).astype(BF16)
            o = jnp.dot(lhs, thl_ref[r, c], preferred_element_type=F32)
            dst[r, :, cut] = o[:ext, :LANES] + (o[:ext, LANES:] + (o[ext:, :LANES] + o[ext:, LANES:]))

    def precond_inner(src, dst, split):
        def body(r, carry):
            precond_row(src, dst, r, split)
            return carry
        lax.fori_loop(1, rows - 1, body, 0)

    def stencil_group(src, dst, r, no_ref, no_i, so_ref, so_i, left, base):
        def body(g, carry):
            s = pl.ds(pl.multiple_of(g * 8, 8), 8)
            ce = src[r, s, :]
            out = (
                wts_ref[r, 0:1, :] * ce
                - wts_ref[r, 1:2, :] * no_ref[no_i, s, :]
                - wts_ref[r, 2:3, :] * so_ref[so_i, s, :]
                - wts_ref[r, 3:4, :] * pltpu.roll(ce, 1, 1)
                - wts_ref[r, 4:5, :] * pltpu.roll(ce, cols - 1, 1)
            )
            dst[r, s, :] = out
            acc_ref[base, s, :] += fold(left[r, s, :] * ce)
            acc_ref[base + 1, s, :] += fold(ce * out)
            return carry
        lax.fori_loop(0, groups, body, 0)

    def stencil_inner(src, dst, left, base):
        def body(r, carry):
            stencil_group(src, dst, r, src, r - 1, src, r + 1, left, base)
            return carry
        lax.fori_loop(1, rows - 1, body, 0)

    def stencil_ends(src, dst, halo, left, base):
        stencil_group(src, dst, 0, halo, 0, src, 1, left, base)
        stencil_group(src, dst, rows - 1, src, rows - 2, halo, 1, left, base)

    def side_copy(src, dst, ssem, rsem, side):
        return pltpu.make_async_remote_copy(
            src_ref=src.at[side], dst_ref=dst.at[1 - side],
            send_sem=ssem.at[side], recv_sem=rsem.at[1 - side],
            device_id={"space": me - 1 if side == 0 else me + 1},
            device_id_type=pl.DeviceIdType.MESH,
        )

    has = (me > 0, me < last)

    precond_row(r0_ref, q_ref, 0, True)
    precond_row(r0_ref, q_ref, rows - 1, True)

    tile_a = lax.shift_right_logical(fa[:pairs] & (cols - 1), 7)
    tile_b = lax.shift_right_logical(fb[:pairs] & (cols - 1), 7)
    for side, r in ((0, 0), (1, rows - 1)):
        va = q_ref[r, :pairs, 0:LANES]
        vb = va
        for c in range(1, tiles):
            x = q_ref[r, :pairs, c * LANES:(c + 1) * LANES]
            va = jnp.where(tile_a == c, x, va)
            vb = jnp.where(tile_b == c, x, vb)
        msg_ref[side, 0:pairs, :] = va
        msg_ref[side, pairs:2 * pairs, :] = vb
        for c in range(tiles):
            cut = slice(c * LANES, (c + 1) * LANES)
            at = 2 * pairs + c
            msg_ref[side, at:at + 1, :] = q_ref[r, pairs:pairs + 1, cut]
            msg_ref[side, at + tiles:at + tiles + 1, :] = active[r:r + 1, cut]
            msg_ref[side, at + 2 * tiles:at + 2 * tiles + 1, :] = valid[r:r + 1, cut]

    pl.semaphore_wait(barrier, last)
    for side in range(2):
        @pl.when(has[side])
        def _():
            side_copy(msg_ref, got_ref, send1, recv1, side).start()

        @pl.when(jnp.logical_not(has[side]))
        def _():
            got_ref[side] = jnp.zeros(got_ref.shape[1:], F32)
            zhalo_ref[side] = jnp.zeros(zhalo_ref.shape[1:], F32)

    precond_inner(r0_ref, q_ref, True)
    stencil_inner(q_ref, w_ref, r0_ref, 0)
    precond_inner(w_ref, z_ref, False)

    def done(src, dst, ssem, rsem):
        for side in range(2):
            @pl.when(has[side])
            def _():
                side_copy(src, dst, ssem, rsem, side).wait_send()
                pltpu.make_async_remote_copy(
                    src_ref=src.at[1 - side], dst_ref=dst.at[side],
                    send_sem=ssem.at[1 - side], recv_sem=rsem.at[side],
                    device_id={"space": me - 1 if side == 0 else me + 1},
                    device_id_type=pl.DeviceIdType.MESH,
                ).wait_recv()

    done(msg_ref, got_ref, send1, recv1)

    def row_of(side, base):
        return jnp.concatenate([got_ref[side, base + c:base + c + 1, :] for c in range(tiles)], 1)

    a_at, v_at = 2 * pairs + tiles, 2 * pairs + 2 * tiles
    set_weights(row_of(0, a_at), row_of(0, v_at), row_of(1, a_at), row_of(1, v_at))
    for side in range(2):
        va = got_ref[side, 0:pairs, :]
        vb = got_ref[side, pairs:2 * pairs, :]
        for c in range(tiles):
            cut = slice(c * LANES, (c + 1) * LANES)
            common = got_ref[side, 2 * pairs + c:2 * pairs + c + 1, :]
            qhalo_ref[side, 0:pairs, cut] = jnp.where(
                tile_a == c, va, jnp.where(tile_b == c, vb, jnp.broadcast_to(common, va.shape))
            )
            qhalo_ref[side, pairs:ext, cut] = jnp.broadcast_to(common, (EXTRA, LANES))

    stencil_ends(q_ref, w_ref, qhalo_ref, r0_ref, 0)
    precond_row(w_ref, z_ref, 0, False)
    precond_row(w_ref, z_ref, rows - 1, False)

    def zcopy(side):
        r = 0 if side == 0 else rows - 1
        return pltpu.make_async_remote_copy(
            src_ref=z_ref.at[r], dst_ref=zhalo_ref.at[1 - side],
            send_sem=send2.at[side], recv_sem=recv2.at[1 - side],
            device_id={"space": me - 1 if side == 0 else me + 1},
            device_id_type=pl.DeviceIdType.MESH,
        )

    def zarrive(side):
        return pltpu.make_async_remote_copy(
            src_ref=z_ref.at[0], dst_ref=zhalo_ref.at[side],
            send_sem=send2.at[1 - side], recv_sem=recv2.at[side],
            device_id={"space": me - 1 if side == 0 else me + 1},
            device_id_type=pl.DeviceIdType.MESH,
        )

    for side in range(2):
        @pl.when(has[side])
        def _():
            zcopy(side).start()

    stencil_inner(z_ref, y_ref, w_ref, 2)

    for side in range(2):
        @pl.when(has[side])
        def _():
            zarrive(side).wait_recv()

    stencil_ends(z_ref, y_ref, zhalo_ref, w_ref, 2)

    lane = lax.broadcasted_iota(jnp.int32, (LANES, LANES), 1)
    table = jnp.zeros((LANES, LANES), F32)
    pad = jnp.zeros((LANES - pairs, 1), F32)
    for i in range(4):
        col = jnp.concatenate([jnp.sum(acc_ref[i, :pairs, :], 1, keepdims=True), pad], 0)
        table = jnp.where(lane == i, jnp.broadcast_to(col, table.shape), table)
    mine = table.T[0:8, :]
    stat_ref[...] = mine

    def stat_copy(slot, peer, k):
        return pltpu.make_async_remote_copy(
            src_ref=stat_ref, dst_ref=all_ref.at[slot],
            send_sem=send3.at[k], recv_sem=recv3.at[k],
            device_id={"space": peer}, device_id_type=pl.DeviceIdType.MESH,
        )

    for k in range(1, count):
        stat_copy(k - 1, lax.rem(me + k, count), k - 1).start()
    for side in range(2):
        @pl.when(has[side])
        def _():
            zcopy(side).wait_send()
    for k in range(1, count):
        stat_copy(k - 1, lax.rem(me + k, count), k - 1).wait()
    total = mine
    for k in range(1, count):
        total = total + all_ref[k - 1]
    back = jnp.concatenate([total, jnp.zeros((LANES - 8, LANES), F32)], 0).T
    gamma0, kappa, mu, nu = (back[:pairs, i:i + 1] for i in range(4))
    a0 = gamma0 / kappa
    gamma1 = a0 * a0 * mu - gamma0
    beta = gamma1 / gamma0
    a1 = gamma1 / (kappa - 2.0 * a0 * mu + a0 * a0 * nu - beta * gamma1 / a0)
    first = a0 + a1 * (1.0 + beta)
    lane_p = lax.broadcasted_iota(jnp.int32, (pairs, LANES), 1)
    coef_ref[...] = jnp.where(lane_p < LANES // 2, first, a0 * a1)


def combine_kernel(smask_ref, scur_ref, focal_ref, coef_ref, q_ref, w_ref, z_ref, y_ref, sol_ref, res_ref):
    rows, block, cols = q_ref.shape
    me = lax.axis_index("space")
    background = smask_ref[...].astype(F32) * scur_ref[...]
    fa, fb = focal_ref[:, 0:1], focal_ref[:, 1:2]
    one = coef_ref[:, 0:1]
    two = coef_ref[:, LANES - 1:LANES]
    for r in range(rows):
        ids = (me * rows + r) * cols + lax.broadcasted_iota(jnp.int32, (block, cols), 1)
        onehot = (ids == fa).astype(F32) - (ids == fb).astype(F32)
        right = background[r:r + 1, :] + FOCAL_CURRENT * onehot
        sol_ref[:, r, :] = one * q_ref[r] - two * z_ref[r]
        res_ref[:, r, :] = right - one * w_ref[r] + two * y_ref[r]


def on_device(count, cond, nodata, gmask, gval, smask, scur, tinv, focal):
    rows, cols = cond.shape
    pairs = focal.shape[0]
    tiles = cols // LANES
    ext = pairs + EXTRA
    field = jax.ShapeDtypeStruct((rows, ext, cols), F32)
    vm = pl.BlockSpec(memory_space=pltpu.VMEM)
    msg = (2, 2 * pairs + 3 * tiles, LANES)
    others = count - 1
    q, w, z, y, coef = pl.pallas_call(
        functools.partial(krylov_kernel, count),
        out_shape=[field] * 4 + [jax.ShapeDtypeStruct((pairs, LANES), F32)],
        in_specs=[vm] * 8,
        out_specs=[vm] * 5,
        scratch_shapes=[
            pltpu.VMEM((rows, ext, cols), F32),
            pltpu.VMEM((rows, tiles, LANES, 2 * LANES), BF16),
            pltpu.VMEM((rows, 8, cols), F32),
            pltpu.VMEM((2, ext, cols), F32),
            pltpu.VMEM((2, ext, cols), F32),
            pltpu.VMEM(msg, F32),
            pltpu.VMEM(msg, F32),
            pltpu.VMEM((4, ext, LANES), F32),
            pltpu.VMEM((8, LANES), F32),
            pltpu.VMEM((others, 8, LANES), F32),
            pltpu.SemaphoreType.DMA((2,)),
            pltpu.SemaphoreType.DMA((2,)),
            pltpu.SemaphoreType.DMA((2,)),
            pltpu.SemaphoreType.DMA((2,)),
            pltpu.SemaphoreType.DMA((others,)),
            pltpu.SemaphoreType.DMA((others,)),
        ],
        compiler_params=pltpu.CompilerParams(
            collective_id=0, has_side_effects=True, vmem_limit_bytes=36 * 1024 * 1024
        ),
        name="krylov",
    )(cond, nodata, gmask, gval, smask, scur, tinv, focal)

    block = 16 if pairs % 16 == 0 else 8
    fspec = pl.BlockSpec((rows, block, cols), lambda i: (0, i, 0))
    whole = pl.BlockSpec((rows, cols), lambda i: (0, 0))
    ospec = pl.BlockSpec((block, rows, cols), lambda i: (i, 0, 0))
    out = jax.ShapeDtypeStruct((pairs, rows, cols), F32)
    return tuple(pl.pallas_call(
        combine_kernel,
        grid=(pairs // block,),
        out_shape=[out, out],
        in_specs=[
            whole, whole,
            pl.BlockSpec((block, 2), lambda i: (i, 0)),
            pl.BlockSpec((block, LANES), lambda i: (i, 0)),
            fspec, fspec, fspec, fspec,
        ],
        out_specs=[ospec, ospec],
        compiler_params=pltpu.CompilerParams(vmem_limit_bytes=20 * 1024 * 1024),
        name="combine",
    )(smask, scur, focal, coef, q, w, z, y))


def solution(mesh):
    return jax.shard_map(
        functools.partial(on_device, mesh.shape["space"]),
        mesh=mesh,
        in_specs=(
            P(("groups", "space"), None),
            P(("groups", "space"), None),
            P(("groups", "space"), None),
            P(("groups", "space"), None),
            P(("groups", "space"), None),
            P(("groups", "space"), None),
            P(("groups", "space"), None, None, None),
            P(("groups", "rhs"), None),
        ),
        out_specs=(P("rhs", ("groups", "space"), None), P("rhs", ("groups", "space"), None)),
        check_vma=False,
    )
```

```python
import functools

import jax
import jax.numpy as jnp
from jax import lax
from jax.experimental import pallas as pl
from jax.experimental.pallas import tpu as pltpu
from jax.sharding import PartitionSpec as P

LEAKAGE = 0.05
FOCAL_CURRENT = 16.0
LANES = 128
EXTRA = 8
F32 = jnp.float32
BF16 = jnp.bfloat16


def fold(x):
    out = x[:, :LANES]
    for c in range(1, x.shape[1] // LANES):
        out = out + x[:, c * LANES:(c + 1) * LANES]
    return out


def krylov_kernel(
    count, cond_hbm, nodata_hbm, gmask_hbm, gval_hbm, smask_hbm, scur_hbm, t_hbm, focal_hbm,
    r0_ref, q_ref, w_ref, z_ref, y_ref, coef_ref,
    cond_ref, nodata_ref, gmask_ref, gval_ref, smask_ref, scur_ref, focal_ref, t_ref,
    thl_ref, wts_ref, qhalo_ref, zhalo_ref, msg_ref, got_ref, acc_ref, stat_ref, all_ref,
    send1, recv1, send2, recv2, send3, recv3, sem_in, sem_t,
):
    rows, cols = cond_ref.shape
    tiles = cols // LANES
    pairs = focal_ref.shape[1]
    ext = pairs + EXTRA
    groups = ext // 8
    me = lax.axis_index("space")
    last = count - 1

    barrier = pltpu.get_barrier_semaphore()
    for off in range(1, count):
        pl.semaphore_signal(
            barrier, inc=1, device_id={"space": lax.rem(me + off, count)},
            device_id_type=pl.DeviceIdType.MESH,
        )

    loads = [
        pltpu.make_async_copy(src, dst, sem_in.at[i])
        for i, (src, dst) in enumerate((
            (focal_hbm, focal_ref), (smask_hbm, smask_ref), (scur_hbm, scur_ref),
            (cond_hbm, cond_ref), (nodata_hbm, nodata_ref), (gmask_hbm, gmask_ref),
            (gval_hbm, gval_ref),
        ))
    ]

    def t_load(r):
        return pltpu.make_async_copy(t_hbm.at[r], t_ref.at[r], sem_t.at[r])

    for load in loads:
        load.start()
    for r in (0, rows - 1, *range(1, rows - 1)):
        t_load(r).start()
    for load in loads:
        load.wait()

    valid = (1 - nodata_ref[...]).astype(F32)
    active = cond_ref[...] * valid
    grounded = gmask_ref[...].astype(F32) * gval_ref[...]
    background = smask_ref[...].astype(F32) * scur_ref[...]

    def set_weights(up_a, up_v, down_a, down_v):
        lane = lax.broadcasted_iota(jnp.int32, (rows, cols), 1)
        zero = jnp.zeros((rows, cols), F32)
        row = lax.broadcasted_iota(jnp.int32, (rows, cols), 0)

        def edge(a, v):
            return 0.5 * (active + a) * valid * v

        def west(x):
            return jnp.where(lane == 0, zero, pltpu.roll(x, 1, 1))

        def east(x):
            return jnp.where(lane == cols - 1, zero, pltpu.roll(x, cols - 1, 1))

        def north(x, h):
            return jnp.where(row == 0, jnp.broadcast_to(h, x.shape), pltpu.roll(x, 1, 0))

        def south(x, h):
            return jnp.where(row == rows - 1, jnp.broadcast_to(h, x.shape), pltpu.roll(x, rows - 1, 0))

        nw = edge(north(active, up_a), north(valid, up_v))
        sw = edge(south(active, down_a), south(valid, down_v))
        ww = edge(west(active), west(valid))
        ew = edge(east(active), east(valid))
        dg = valid * (LEAKAGE + grounded) + (1.0 - valid) + nw + sw + ww + ew
        for r in range(rows):
            for i, x in enumerate((dg, nw, sw, ww, ew)):
                wts_ref[r, i:i + 1, :] = x[r:r + 1, :]

    acc_ref[...] = jnp.zeros(acc_ref.shape, F32)
    diagonal = lax.broadcasted_iota(jnp.int32, (ext, pairs), 0) == lax.broadcasted_iota(
        jnp.int32, (ext, pairs), 1)
    is_pair = lax.broadcasted_iota(jnp.int32, (ext, 1), 0) < pairs

    def column(i):
        line = jnp.broadcast_to(focal_ref[i:i + 1, :].astype(F32), (ext, pairs))
        at = jnp.sum(jnp.where(diagonal, line, 0.0), 1, keepdims=True).astype(jnp.int32)
        return jnp.where(is_pair, at, -1)

    fa, fb = column(0), column(1)

    def right_side(r):
        ids = (me * rows + r) * cols + lax.broadcasted_iota(jnp.int32, (ext, cols), 1)
        onehot = (ids == fa).astype(F32) - (ids == fb).astype(F32)
        r0_ref[r] = background[r:r + 1, :] + FOCAL_CURRENT * onehot

    right_side(0)
    right_side(rows - 1)

    def precond_row(src, dst, r, split):
        for c in range(tiles):
            cut = slice(c * LANES, (c + 1) * LANES)
            if split:
                t = t_ref[r, c]
                thi = t.astype(BF16)
                thl_ref[r, c, :, :LANES] = thi
                thl_ref[r, c, :, LANES:] = (t - thi.astype(F32)).astype(BF16)
            x = src[r, :, cut]
            hi = x.astype(BF16).astype(F32)
            lhs = jnp.concatenate([hi, x - hi], 0).astype(BF16)
            o = jnp.dot(lhs, thl_ref[r, c], preferred_element_type=F32)
            dst[r, :, cut] = o[:ext, :LANES] + (o[:ext, LANES:] + (o[ext:, :LANES] + o[ext:, LANES:]))

    def precond_inner(src, dst, split):
        def body(r, carry):
            if split:
                t_load(r).wait()
            precond_row(src, dst, r, split)
            return carry
        lax.fori_loop(1, rows - 1, body, 0)

    def stencil_group(src, dst, r, no_ref, no_i, so_ref, so_i, left, base):
        def body(g, carry):
            s = pl.ds(pl.multiple_of(g * 8, 8), 8)
            ce = src[r, s, :]
            out = (
                wts_ref[r, 0:1, :] * ce
                - wts_ref[r, 1:2, :] * no_ref[no_i, s, :]
                - wts_ref[r, 2:3, :] * so_ref[so_i, s, :]
                - wts_ref[r, 3:4, :] * pltpu.roll(ce, 1, 1)
                - wts_ref[r, 4:5, :] * pltpu.roll(ce, cols - 1, 1)
            )
            dst[r, s, :] = out
            acc_ref[base, s, :] += fold(left[r, s, :] * ce)
            acc_ref[base + 1, s, :] += fold(ce * out)
            return carry
        lax.fori_loop(0, groups, body, 0)

    def stencil_inner(src, dst, left, base):
        def body(r, carry):
            stencil_group(src, dst, r, src, r - 1, src, r + 1, left, base)
            return carry
        lax.fori_loop(1, rows - 1, body, 0)

    def stencil_ends(src, dst, halo, left, base):
        stencil_group(src, dst, 0, halo, 0, src, 1, left, base)
        stencil_group(src, dst, rows - 1, src, rows - 2, halo, 1, left, base)

    def side_copy(src, dst, ssem, rsem, side):
        return pltpu.make_async_remote_copy(
            src_ref=src.at[side], dst_ref=dst.at[1 - side],
            send_sem=ssem.at[side], recv_sem=rsem.at[1 - side],
            device_id={"space": me - 1 if side == 0 else me + 1},
            device_id_type=pl.DeviceIdType.MESH,
        )

    has = (me > 0, me < last)

    for r in (0, rows - 1):
        t_load(r).wait()
        precond_row(r0_ref, q_ref, r, True)

    tile_a = lax.shift_right_logical(fa[:pairs] & (cols - 1), 7)
    tile_b = lax.shift_right_logical(fb[:pairs] & (cols - 1), 7)
    for side, r in ((0, 0), (1, rows - 1)):
        va = q_ref[r, :pairs, 0:LANES]
        vb = va
        for c in range(1, tiles):
            x = q_ref[r, :pairs, c * LANES:(c + 1) * LANES]
            va = jnp.where(tile_a == c, x, va)
            vb = jnp.where(tile_b == c, x, vb)
        msg_ref[side, 0:pairs, :] = va
        msg_ref[side, pairs:2 * pairs, :] = vb
        for c in range(tiles):
            cut = slice(c * LANES, (c + 1) * LANES)
            at = 2 * pairs + c
            msg_ref[side, at:at + 1, :] = q_ref[r, pairs:pairs + 1, cut]
            msg_ref[side, at + tiles:at + tiles + 1, :] = active[r:r + 1, cut]
            msg_ref[side, at + 2 * tiles:at + 2 * tiles + 1, :] = valid[r:r + 1, cut]

    pl.semaphore_wait(barrier, last)
    for side in range(2):
        @pl.when(has[side])
        def _():
            side_copy(msg_ref, got_ref, send1, recv1, side).start()

        @pl.when(jnp.logical_not(has[side]))
        def _():
            got_ref[side] = jnp.zeros(got_ref.shape[1:], F32)
            zhalo_ref[side] = jnp.zeros(zhalo_ref.shape[1:], F32)

    none = jnp.zeros((1, cols), F32)
    set_weights(none, none, none, none)
    for r in range(1, rows - 1):
        right_side(r)
    precond_inner(r0_ref, q_ref, True)
    stencil_inner(q_ref, w_ref, r0_ref, 0)

    def done(src, dst, ssem, rsem):
        for side in range(2):
            @pl.when(has[side])
            def _():
                side_copy(src, dst, ssem, rsem, side).wait_send()
                pltpu.make_async_remote_copy(
                    src_ref=src.at[1 - side], dst_ref=dst.at[side],
                    send_sem=ssem.at[1 - side], recv_sem=rsem.at[side],
                    device_id={"space": me - 1 if side == 0 else me + 1},
                    device_id_type=pl.DeviceIdType.MESH,
                ).wait_recv()

    done(msg_ref, got_ref, send1, recv1)

    def row_of(side, base):
        return jnp.concatenate([got_ref[side, base + c:base + c + 1, :] for c in range(tiles)], 1)

    a_at, v_at = 2 * pairs + tiles, 2 * pairs + 2 * tiles
    set_weights(row_of(0, a_at), row_of(0, v_at), row_of(1, a_at), row_of(1, v_at))
    for side in range(2):
        va = got_ref[side, 0:pairs, :]
        vb = got_ref[side, pairs:2 * pairs, :]
        for c in range(tiles):
            cut = slice(c * LANES, (c + 1) * LANES)
            common = got_ref[side, 2 * pairs + c:2 * pairs + c + 1, :]
            qhalo_ref[side, 0:pairs, cut] = jnp.where(
                tile_a == c, va, jnp.where(tile_b == c, vb, jnp.broadcast_to(common, va.shape))
            )
            qhalo_ref[side, pairs:ext, cut] = jnp.broadcast_to(common, (EXTRA, LANES))

    stencil_ends(q_ref, w_ref, qhalo_ref, r0_ref, 0)
    precond_row(w_ref, z_ref, 0, False)
    precond_row(w_ref, z_ref, rows - 1, False)

    def zcopy(side):
        r = 0 if side == 0 else rows - 1
        return pltpu.make_async_remote_copy(
            src_ref=z_ref.at[r], dst_ref=zhalo_ref.at[1 - side],
            send_sem=send2.at[side], recv_sem=recv2.at[1 - side],
            device_id={"space": me - 1 if side == 0 else me + 1},
            device_id_type=pl.DeviceIdType.MESH,
        )

    def zarrive(side):
        return pltpu.make_async_remote_copy(
            src_ref=z_ref.at[0], dst_ref=zhalo_ref.at[side],
            send_sem=send2.at[1 - side], recv_sem=recv2.at[side],
            device_id={"space": me - 1 if side == 0 else me + 1},
            device_id_type=pl.DeviceIdType.MESH,
        )

    for side in range(2):
        @pl.when(has[side])
        def _():
            zcopy(side).start()

    precond_inner(w_ref, z_ref, False)
    stencil_inner(z_ref, y_ref, w_ref, 2)

    for side in range(2):
        @pl.when(has[side])
        def _():
            zarrive(side).wait_recv()

    stencil_ends(z_ref, y_ref, zhalo_ref, w_ref, 2)

    lane = lax.broadcasted_iota(jnp.int32, (LANES, LANES), 1)
    table = jnp.zeros((LANES, LANES), F32)
    pad = jnp.zeros((LANES - pairs, 1), F32)
    for i in range(4):
        col = jnp.concatenate([jnp.sum(acc_ref[i, :pairs, :], 1, keepdims=True), pad], 0)
        table = jnp.where(lane == i, jnp.broadcast_to(col, table.shape), table)
    mine = table.T[0:8, :]
    stat_ref[...] = mine

    def stat_copy(slot, peer, k):
        return pltpu.make_async_remote_copy(
            src_ref=stat_ref, dst_ref=all_ref.at[slot],
            send_sem=send3.at[k], recv_sem=recv3.at[k],
            device_id={"space": peer}, device_id_type=pl.DeviceIdType.MESH,
        )

    for k in range(1, count):
        stat_copy(k - 1, lax.rem(me + k, count), k - 1).start()
    for side in range(2):
        @pl.when(has[side])
        def _():
            zcopy(side).wait_send()
    for k in range(1, count):
        stat_copy(k - 1, lax.rem(me + k, count), k - 1).wait()
    total = mine
    for k in range(1, count):
        total = total + all_ref[k - 1]
    back = jnp.concatenate([total, jnp.zeros((LANES - 8, LANES), F32)], 0).T
    gamma0, kappa, mu, nu = (back[:pairs, i:i + 1] for i in range(4))
    a0 = gamma0 / kappa
    gamma1 = a0 * a0 * mu - gamma0
    beta = gamma1 / gamma0
    a1 = gamma1 / (kappa - 2.0 * a0 * mu + a0 * a0 * nu - beta * gamma1 / a0)
    first = a0 + a1 * (1.0 + beta)
    lane_p = lax.broadcasted_iota(jnp.int32, (pairs, LANES), 1)
    coef_ref[...] = jnp.where(lane_p < LANES // 2, first, a0 * a1)


def combine_kernel(coef_ref, r0_ref, q_ref, w_ref, z_ref, y_ref, sol_hbm, res_hbm, sol_ref, res_ref, sem):
    pairs, rows, cols = sol_ref.shape
    block = 8

    def out(i, src, dst, k):
        cut = pl.ds(pl.multiple_of(i * block, block), block)
        return pltpu.make_async_copy(src.at[cut], dst.at[cut], sem.at[k, i])

    def body(i, carry):
        cut = pl.ds(pl.multiple_of(i * block, block), block)
        one = coef_ref[cut, 0:1]
        two = coef_ref[cut, LANES - 1:LANES]
        for r in range(rows):
            sol_ref[cut, r, :] = one * q_ref[r, cut, :] - two * z_ref[r, cut, :]
            res_ref[cut, r, :] = r0_ref[r, cut, :] - one * w_ref[r, cut, :] + two * y_ref[r, cut, :]
        out(i, sol_ref, sol_hbm, 0).start()
        out(i, res_ref, res_hbm, 1).start()
        return carry

    lax.fori_loop(0, pairs // block, body, 0)

    def finish(i, carry):
        out(i, sol_ref, sol_hbm, 0).wait()
        out(i, res_ref, res_hbm, 1).wait()
        return carry

    lax.fori_loop(0, pairs // block, finish, 0)


def on_device(count, cond, nodata, gmask, gval, smask, scur, tinv, focal):
    rows, cols = cond.shape
    pairs = focal.shape[0]
    tiles = cols // LANES
    ext = pairs + EXTRA
    field = jax.ShapeDtypeStruct((rows, ext, cols), F32)
    vm = pl.BlockSpec(memory_space=pltpu.VMEM)
    hbm = pl.BlockSpec(memory_space=pltpu.HBM)
    msg = (2, 2 * pairs + 3 * tiles, LANES)
    others = count - 1
    small = (rows, cols)
    r0, q, w, z, y, coef = pl.pallas_call(
        functools.partial(krylov_kernel, count),
        out_shape=[field] * 5 + [jax.ShapeDtypeStruct((pairs, LANES), F32)],
        in_specs=[hbm] * 8,
        out_specs=[vm] * 6,
        scratch_shapes=[
            pltpu.VMEM(small, F32),
            pltpu.VMEM(small, jnp.int32),
            pltpu.VMEM(small, jnp.int32),
            pltpu.VMEM(small, F32),
            pltpu.VMEM(small, jnp.int32),
            pltpu.VMEM(small, F32),
            pltpu.VMEM((2, pairs), jnp.int32),
            pltpu.VMEM(tinv.shape, F32),
            pltpu.VMEM((rows, tiles, LANES, 2 * LANES), BF16),
            pltpu.VMEM((rows, 8, cols), F32),
            pltpu.VMEM((2, ext, cols), F32),
            pltpu.VMEM((2, ext, cols), F32),
            pltpu.VMEM(msg, F32),
            pltpu.VMEM(msg, F32),
            pltpu.VMEM((4, ext, LANES), F32),
            pltpu.VMEM((8, LANES), F32),
            pltpu.VMEM((others, 8, LANES), F32),
            pltpu.SemaphoreType.DMA((2,)),
            pltpu.SemaphoreType.DMA((2,)),
            pltpu.SemaphoreType.DMA((2,)),
            pltpu.SemaphoreType.DMA((2,)),
            pltpu.SemaphoreType.DMA((others,)),
            pltpu.SemaphoreType.DMA((others,)),
            pltpu.SemaphoreType.DMA((7,)),
            pltpu.SemaphoreType.DMA((rows,)),
        ],
        compiler_params=pltpu.CompilerParams(
            collective_id=0, has_side_effects=True, vmem_limit_bytes=36 * 1024 * 1024
        ),
        name="krylov",
    )(*(
        pltpu.with_memory_space_constraint(x, pltpu.HBM)
        for x in (cond, nodata, gmask, gval, smask, scur, tinv, focal.T)
    ))

    out = jax.ShapeDtypeStruct((pairs, rows, cols), F32)
    return tuple(pl.pallas_call(
        combine_kernel,
        out_shape=[out, out],
        in_specs=[vm] * 6,
        out_specs=[hbm, hbm],
        scratch_shapes=[
            pltpu.VMEM(out.shape, F32),
            pltpu.VMEM(out.shape, F32),
            pltpu.SemaphoreType.DMA((2, pairs // 8)),
        ],
        compiler_params=pltpu.CompilerParams(vmem_limit_bytes=20 * 1024 * 1024),
        name="combine",
    )(coef, r0, q, w, z, y))


def solution(mesh):
    return jax.shard_map(
        functools.partial(on_device, mesh.shape["space"]),
        mesh=mesh,
        in_specs=(
            P(("groups", "space"), None),
            P(("groups", "space"), None),
            P(("groups", "space"), None),
            P(("groups", "space"), None),
            P(("groups", "space"), None),
            P(("groups", "space"), None),
            P(("groups", "space"), None, None, None),
            P(("groups", "rhs"), None),
        ),
        out_specs=(P("rhs", ("groups", "space"), None), P("rhs", ("groups", "space"), None)),
        check_vma=False,
    )
```

```python
import functools

import jax
import jax.numpy as jnp
from jax import lax
from jax.experimental import pallas as pl
from jax.experimental.pallas import tpu as pltpu
from jax.sharding import PartitionSpec as P

LEAKAGE = 0.05
FOCAL_CURRENT = 16.0
LANES = 128
EXTRA = 8
F32 = jnp.float32
BF16 = jnp.bfloat16


def fold(x):
    out = x[:, :LANES]
    for c in range(1, x.shape[1] // LANES):
        out = out + x[:, c * LANES:(c + 1) * LANES]
    return out


def krylov_kernel(
    count, cond_hbm, nodata_hbm, gmask_hbm, gval_hbm, smask_hbm, scur_hbm, t_hbm, focal_hbm,
    r0_ref, q_ref, w_ref, z_ref, y_ref, coef_ref,
    cond_ref, nodata_ref, gmask_ref, gval_ref, smask_ref, scur_ref, focal_ref, t_ref,
    thl_ref, wts_ref, qhalo_ref, zhalo_ref, msg_ref, got_ref, zmsg_ref, zgot_ref, acc_ref, stat_ref, all_ref,
    send1, recv1, send2, recv2, send3, recv3, sem_in, sem_t,
):
    rows, cols = cond_ref.shape
    tiles = cols // LANES
    pairs = focal_ref.shape[1]
    ext = pairs + EXTRA
    groups = ext // 8
    me = lax.axis_index("space")
    last = count - 1

    barrier = pltpu.get_barrier_semaphore()
    for off in range(1, count):
        pl.semaphore_signal(
            barrier, inc=1, device_id={"space": lax.rem(me + off, count)},
            device_id_type=pl.DeviceIdType.MESH,
        )

    loads = [
        pltpu.make_async_copy(src, dst, sem_in.at[i])
        for i, (src, dst) in enumerate((
            (focal_hbm, focal_ref), (smask_hbm, smask_ref), (scur_hbm, scur_ref),
            (cond_hbm, cond_ref), (nodata_hbm, nodata_ref), (gmask_hbm, gmask_ref),
            (gval_hbm, gval_ref),
        ))
    ]

    def t_load(r):
        return pltpu.make_async_copy(t_hbm.at[r], t_ref.at[r], sem_t.at[r])

    for load in loads:
        load.start()
    for r in (0, rows - 1, *range(1, rows - 1)):
        t_load(r).start()
    for load in loads:
        load.wait()

    valid = (1 - nodata_ref[...]).astype(F32)
    active = cond_ref[...] * valid
    grounded = gmask_ref[...].astype(F32) * gval_ref[...]
    background = smask_ref[...].astype(F32) * scur_ref[...]

    def set_weights(up_a, up_v, down_a, down_v):
        lane = lax.broadcasted_iota(jnp.int32, (rows, cols), 1)
        zero = jnp.zeros((rows, cols), F32)
        row = lax.broadcasted_iota(jnp.int32, (rows, cols), 0)

        def edge(a, v):
            return 0.5 * (active + a) * valid * v

        def west(x):
            return jnp.where(lane == 0, zero, pltpu.roll(x, 1, 1))

        def east(x):
            return jnp.where(lane == cols - 1, zero, pltpu.roll(x, cols - 1, 1))

        def north(x, h):
            return jnp.where(row == 0, jnp.broadcast_to(h, x.shape), pltpu.roll(x, 1, 0))

        def south(x, h):
            return jnp.where(row == rows - 1, jnp.broadcast_to(h, x.shape), pltpu.roll(x, rows - 1, 0))

        nw = edge(north(active, up_a), north(valid, up_v))
        sw = edge(south(active, down_a), south(valid, down_v))
        ww = edge(west(active), west(valid))
        ew = edge(east(active), east(valid))
        dg = valid * (LEAKAGE + grounded) + (1.0 - valid) + nw + sw + ww + ew
        for r in range(rows):
            for i, x in enumerate((dg, nw, sw, ww, ew)):
                wts_ref[r, i:i + 1, :] = x[r:r + 1, :]

    acc_ref[...] = jnp.zeros(acc_ref.shape, F32)
    diagonal = lax.broadcasted_iota(jnp.int32, (ext, pairs), 0) == lax.broadcasted_iota(
        jnp.int32, (ext, pairs), 1)
    is_pair = lax.broadcasted_iota(jnp.int32, (ext, 1), 0) < pairs

    def column(i):
        line = jnp.broadcast_to(focal_ref[i:i + 1, :].astype(F32), (ext, pairs))
        at = jnp.sum(jnp.where(diagonal, line, 0.0), 1, keepdims=True).astype(jnp.int32)
        return jnp.where(is_pair, at, -1)

    fa, fb = column(0), column(1)

    def right_side(r):
        ids = (me * rows + r) * cols + lax.broadcasted_iota(jnp.int32, (ext, cols), 1)
        onehot = (ids == fa).astype(F32) - (ids == fb).astype(F32)
        r0_ref[r] = background[r:r + 1, :] + FOCAL_CURRENT * onehot

    right_side(0)
    right_side(rows - 1)

    def precond_row(src, dst, r, split):
        for c in range(tiles):
            cut = slice(c * LANES, (c + 1) * LANES)
            if split:
                t = t_ref[r, c]
                thi = t.astype(BF16)
                thl_ref[r, c, :, :LANES] = thi
                thl_ref[r, c, :, LANES:] = (t - thi.astype(F32)).astype(BF16)
            x = src[r, :, cut]
            hi = x.astype(BF16).astype(F32)
            lhs = jnp.concatenate([hi, x - hi], 0).astype(BF16)
            o = jnp.dot(lhs, thl_ref[r, c], preferred_element_type=F32)
            dst[r, :, cut] = o[:ext, :LANES] + (o[:ext, LANES:] + (o[ext:, :LANES] + o[ext:, LANES:]))

    def precond_inner(src, dst, split):
        def body(r, carry):
            if split:
                t_load(r).wait()
            precond_row(src, dst, r, split)
            return carry
        lax.fori_loop(1, rows - 1, body, 0)

    def stencil_group(src, dst, r, no_ref, no_i, so_ref, so_i, left, base):
        def body(g, carry):
            s = pl.ds(pl.multiple_of(g * 8, 8), 8)
            ce = src[r, s, :]
            out = (
                wts_ref[r, 0:1, :] * ce
                - wts_ref[r, 1:2, :] * no_ref[no_i, s, :]
                - wts_ref[r, 2:3, :] * so_ref[so_i, s, :]
                - wts_ref[r, 3:4, :] * pltpu.roll(ce, 1, 1)
                - wts_ref[r, 4:5, :] * pltpu.roll(ce, cols - 1, 1)
            )
            dst[r, s, :] = out
            acc_ref[base, s, :] += fold(left[r, s, :] * ce)
            acc_ref[base + 1, s, :] += fold(ce * out)
            return carry
        lax.fori_loop(0, groups, body, 0, unroll=3 if groups % 3 == 0 else 1)

    def stencil_inner(src, dst, left, base):
        def body(r, carry):
            stencil_group(src, dst, r, src, r - 1, src, r + 1, left, base)
            return carry
        lax.fori_loop(1, rows - 1, body, 0)

    def stencil_ends(src, dst, halo, left, base):
        stencil_group(src, dst, 0, halo, 0, src, 1, left, base)
        stencil_group(src, dst, rows - 1, src, rows - 2, halo, 1, left, base)

    def side_copy(src, dst, ssem, rsem, side):
        return pltpu.make_async_remote_copy(
            src_ref=src.at[side], dst_ref=dst.at[1 - side],
            send_sem=ssem.at[side], recv_sem=rsem.at[1 - side],
            device_id={"space": me - 1 if side == 0 else me + 1},
            device_id_type=pl.DeviceIdType.MESH,
        )

    has = (me > 0, me < last)

    for r in (0, rows - 1):
        t_load(r).wait()
        precond_row(r0_ref, q_ref, r, True)

    tile_a = lax.shift_right_logical(fa[:pairs] & (cols - 1), 7)
    tile_b = lax.shift_right_logical(fb[:pairs] & (cols - 1), 7)
    def pack(src, r, dst, side):
        va = src[r, :pairs, 0:LANES]
        vb = va
        for c in range(1, tiles):
            x = src[r, :pairs, c * LANES:(c + 1) * LANES]
            va = jnp.where(tile_a == c, x, va)
            vb = jnp.where(tile_b == c, x, vb)
        dst[side, 0:pairs, :] = va
        dst[side, pairs:2 * pairs, :] = vb
        for c in range(tiles):
            at = 2 * pairs + c
            dst[side, at:at + 1, :] = src[r, pairs:pairs + 1, c * LANES:(c + 1) * LANES]

    for side, r in ((0, 0), (1, rows - 1)):
        pack(q_ref, r, msg_ref, side)
        for c in range(tiles):
            cut = slice(c * LANES, (c + 1) * LANES)
            at = 2 * pairs + c
            msg_ref[side, at + tiles:at + tiles + 1, :] = active[r:r + 1, cut]
            msg_ref[side, at + 2 * tiles:at + 2 * tiles + 1, :] = valid[r:r + 1, cut]
            msg_ref[side, at + 3 * tiles:at + 3 * tiles + 1, :] = t_ref[r, c, 0:1, :]
            msg_ref[side, at + 4 * tiles:at + 4 * tiles + 1, :] = t_ref[r, c, LANES - 1:LANES, :]

    pl.semaphore_wait(barrier, last)
    for side in range(2):
        @pl.when(has[side])
        def _():
            side_copy(msg_ref, got_ref, send1, recv1, side).start()

        @pl.when(jnp.logical_not(has[side]))
        def _():
            got_ref[side] = jnp.zeros(got_ref.shape[1:], F32)
            zgot_ref[side] = jnp.zeros(zgot_ref.shape[1:], F32)

    none = jnp.zeros((1, cols), F32)
    set_weights(none, none, none, none)
    for r in range(1, rows - 1):
        right_side(r)
    precond_inner(r0_ref, q_ref, True)
    stencil_inner(q_ref, w_ref, r0_ref, 0)

    def done(src, dst, ssem, rsem):
        for side in range(2):
            @pl.when(has[side])
            def _():
                side_copy(src, dst, ssem, rsem, side).wait_send()
                pltpu.make_async_remote_copy(
                    src_ref=src.at[1 - side], dst_ref=dst.at[side],
                    send_sem=ssem.at[1 - side], recv_sem=rsem.at[side],
                    device_id={"space": me - 1 if side == 0 else me + 1},
                    device_id_type=pl.DeviceIdType.MESH,
                ).wait_recv()

    done(msg_ref, got_ref, send1, recv1)

    def row_of(side, base):
        return jnp.concatenate([got_ref[side, base + c:base + c + 1, :] for c in range(tiles)], 1)

    a_at, v_at = 2 * pairs + tiles, 2 * pairs + 2 * tiles
    set_weights(row_of(0, a_at), row_of(0, v_at), row_of(1, a_at), row_of(1, v_at))
    for side in range(2):
        va = got_ref[side, 0:pairs, :]
        vb = got_ref[side, pairs:2 * pairs, :]
        for c in range(tiles):
            cut = slice(c * LANES, (c + 1) * LANES)
            common = got_ref[side, 2 * pairs + c:2 * pairs + c + 1, :]
            qhalo_ref[side, 0:pairs, cut] = jnp.where(
                tile_a == c, va, jnp.where(tile_b == c, vb, jnp.broadcast_to(common, va.shape))
            )
            qhalo_ref[side, pairs:ext, cut] = jnp.broadcast_to(common, (EXTRA, LANES))

    stencil_ends(q_ref, w_ref, qhalo_ref, r0_ref, 0)
    precond_row(w_ref, z_ref, 0, False)
    precond_row(w_ref, z_ref, rows - 1, False)

    ends_at = 2 * pairs + tiles
    lane_e = lax.broadcasted_iota(jnp.int32, (pairs, LANES), 1)
    for side, r in ((0, 0), (1, rows - 1)):
        pack(z_ref, r, zmsg_ref, side)
        ends = jnp.zeros((pairs, LANES), F32)
        for c in range(tiles):
            cut = slice(c * LANES, (c + 1) * LANES)
            diff = w_ref[r, :pairs, cut] - w_ref[r, pairs:pairs + 1, cut]
            ends = jnp.where(lane_e == c, jnp.broadcast_to(diff[:, 0:1], ends.shape), ends)
            ends = jnp.where(lane_e == tiles + c, jnp.broadcast_to(diff[:, LANES - 1:], ends.shape), ends)
        zmsg_ref[side, ends_at:ends_at + pairs, :] = ends

    for side in range(2):
        @pl.when(has[side])
        def _():
            side_copy(zmsg_ref, zgot_ref, send2, recv2, side).start()

    precond_inner(w_ref, z_ref, False)
    stencil_inner(z_ref, y_ref, w_ref, 2)

    done(zmsg_ref, zgot_ref, send2, recv2)
    for side in range(2):
        va = zgot_ref[side, 0:pairs, :]
        vb = zgot_ref[side, pairs:2 * pairs, :]
        ends = zgot_ref[side, ends_at:ends_at + pairs, :]
        for c in range(tiles):
            cut = slice(c * LANES, (c + 1) * LANES)
            common = zgot_ref[side, 2 * pairs + c:2 * pairs + c + 1, :]
            at = 2 * pairs + 3 * tiles + c
            other = (
                common
                + ends[:, c:c + 1] * got_ref[side, at:at + 1, :]
                + ends[:, tiles + c:tiles + c + 1] * got_ref[side, at + tiles:at + tiles + 1, :]
            )
            zhalo_ref[side, 0:pairs, cut] = jnp.where(tile_a == c, va, jnp.where(tile_b == c, vb, other))
            zhalo_ref[side, pairs:ext, cut] = jnp.broadcast_to(common, (EXTRA, LANES))

    stencil_ends(z_ref, y_ref, zhalo_ref, w_ref, 2)

    lane = lax.broadcasted_iota(jnp.int32, (LANES, LANES), 1)
    table = jnp.zeros((LANES, LANES), F32)
    pad = jnp.zeros((LANES - pairs, 1), F32)
    for i in range(4):
        col = jnp.concatenate([jnp.sum(acc_ref[i, :pairs, :], 1, keepdims=True), pad], 0)
        table = jnp.where(lane == i, jnp.broadcast_to(col, table.shape), table)
    mine = table.T[0:8, :]
    stat_ref[...] = mine

    def stat_copy(slot, peer, k):
        return pltpu.make_async_remote_copy(
            src_ref=stat_ref, dst_ref=all_ref.at[slot],
            send_sem=send3.at[k], recv_sem=recv3.at[k],
            device_id={"space": peer}, device_id_type=pl.DeviceIdType.MESH,
        )

    for k in range(1, count):
        stat_copy(k - 1, lax.rem(me + k, count), k - 1).start()
    for k in range(1, count):
        stat_copy(k - 1, lax.rem(me + k, count), k - 1).wait()
    total = mine
    for k in range(1, count):
        total = total + all_ref[k - 1]
    back = jnp.concatenate([total, jnp.zeros((LANES - 8, LANES), F32)], 0).T
    gamma0, kappa, mu, nu = (back[:pairs, i:i + 1] for i in range(4))
    a0 = gamma0 / kappa
    gamma1 = a0 * a0 * mu - gamma0
    beta = gamma1 / gamma0
    a1 = gamma1 / (kappa - 2.0 * a0 * mu + a0 * a0 * nu - beta * gamma1 / a0)
    first = a0 + a1 * (1.0 + beta)
    lane_p = lax.broadcasted_iota(jnp.int32, (pairs, LANES), 1)
    coef_ref[...] = jnp.where(lane_p < LANES // 2, first, a0 * a1)


def combine_kernel(coef_ref, r0_ref, q_ref, w_ref, z_ref, y_ref, sol_hbm, res_hbm, sol_ref, res_ref, sem):
    pairs, rows, cols = sol_ref.shape
    block = 8

    def out(i, src, dst, k):
        cut = pl.ds(pl.multiple_of(i * block, block), block)
        return pltpu.make_async_copy(src.at[cut], dst.at[cut], sem.at[k, i])

    def body(i, carry):
        cut = pl.ds(pl.multiple_of(i * block, block), block)
        one = coef_ref[cut, 0:1]
        two = coef_ref[cut, LANES - 1:LANES]
        for r in range(rows):
            sol_ref[cut, r, :] = one * q_ref[r, cut, :] - two * z_ref[r, cut, :]
            res_ref[cut, r, :] = r0_ref[r, cut, :] - one * w_ref[r, cut, :] + two * y_ref[r, cut, :]
        out(i, sol_ref, sol_hbm, 0).start()
        out(i, res_ref, res_hbm, 1).start()
        return carry

    lax.fori_loop(0, pairs // block, body, 0)

    def finish(i, carry):
        out(i, sol_ref, sol_hbm, 0).wait()
        out(i, res_ref, res_hbm, 1).wait()
        return carry

    lax.fori_loop(0, pairs // block, finish, 0)


def on_device(count, cond, nodata, gmask, gval, smask, scur, tinv, focal):
    rows, cols = cond.shape
    pairs = focal.shape[0]
    tiles = cols // LANES
    ext = pairs + EXTRA
    field = jax.ShapeDtypeStruct((rows, ext, cols), F32)
    vm = pl.BlockSpec(memory_space=pltpu.VMEM)
    hbm = pl.BlockSpec(memory_space=pltpu.HBM)
    msg = (2, 2 * pairs + 5 * tiles, LANES)
    zmsg = (2, 3 * pairs + tiles, LANES)
    others = count - 1
    small = (rows, cols)
    r0, q, w, z, y, coef = pl.pallas_call(
        functools.partial(krylov_kernel, count),
        out_shape=[field] * 5 + [jax.ShapeDtypeStruct((pairs, LANES), F32)],
        in_specs=[hbm] * 8,
        out_specs=[vm] * 6,
        scratch_shapes=[
            pltpu.VMEM(small, F32),
            pltpu.VMEM(small, jnp.int32),
            pltpu.VMEM(small, jnp.int32),
            pltpu.VMEM(small, F32),
            pltpu.VMEM(small, jnp.int32),
            pltpu.VMEM(small, F32),
            pltpu.VMEM((2, pairs), jnp.int32),
            pltpu.VMEM(tinv.shape, F32),
            pltpu.VMEM((rows, tiles, LANES, 2 * LANES), BF16),
            pltpu.VMEM((rows, 8, cols), F32),
            pltpu.VMEM((2, ext, cols), F32),
            pltpu.VMEM((2, ext, cols), F32),
            pltpu.VMEM(msg, F32),
            pltpu.VMEM(msg, F32),
            pltpu.VMEM(zmsg, F32),
            pltpu.VMEM(zmsg, F32),
            pltpu.VMEM((4, ext, LANES), F32),
            pltpu.VMEM((8, LANES), F32),
            pltpu.VMEM((others, 8, LANES), F32),
            pltpu.SemaphoreType.DMA((2,)),
            pltpu.SemaphoreType.DMA((2,)),
            pltpu.SemaphoreType.DMA((2,)),
            pltpu.SemaphoreType.DMA((2,)),
            pltpu.SemaphoreType.DMA((others,)),
            pltpu.SemaphoreType.DMA((others,)),
            pltpu.SemaphoreType.DMA((7,)),
            pltpu.SemaphoreType.DMA((rows,)),
        ],
        compiler_params=pltpu.CompilerParams(
            collective_id=0, has_side_effects=True, vmem_limit_bytes=36 * 1024 * 1024
        ),
        name="krylov",
    )(*(
        pltpu.with_memory_space_constraint(x, pltpu.HBM)
        for x in (cond, nodata, gmask, gval, smask, scur, tinv, focal.T)
    ))

    out = jax.ShapeDtypeStruct((pairs, rows, cols), F32)
    return tuple(pl.pallas_call(
        combine_kernel,
        out_shape=[out, out],
        in_specs=[vm] * 6,
        out_specs=[hbm, hbm],
        scratch_shapes=[
            pltpu.VMEM(out.shape, F32),
            pltpu.VMEM(out.shape, F32),
            pltpu.SemaphoreType.DMA((2, pairs // 8)),
        ],
        compiler_params=pltpu.CompilerParams(vmem_limit_bytes=20 * 1024 * 1024),
        name="combine",
    )(coef, r0, q, w, z, y))


def solution(mesh):
    return jax.shard_map(
        functools.partial(on_device, mesh.shape["space"]),
        mesh=mesh,
        in_specs=(
            P(("groups", "space"), None),
            P(("groups", "space"), None),
            P(("groups", "space"), None),
            P(("groups", "space"), None),
            P(("groups", "space"), None),
            P(("groups", "space"), None),
            P(("groups", "space"), None, None, None),
            P(("groups", "rhs"), None),
        ),
        out_specs=(P("rhs", ("groups", "space"), None), P("rhs", ("groups", "space"), None)),
        check_vma=False,
    )
```

```python
import functools

import jax
import jax.numpy as jnp
from jax import lax
from jax.experimental import pallas as pl
from jax.experimental.pallas import tpu as pltpu
from jax.sharding import PartitionSpec as P

LEAKAGE = 0.05
FOCAL_CURRENT = 16.0
LANES = 128
EXTRA = 8
F32 = jnp.float32
BF16 = jnp.bfloat16


def fold(x):
    out = x[:, :LANES]
    for c in range(1, x.shape[1] // LANES):
        out = out + x[:, c * LANES:(c + 1) * LANES]
    return out


def krylov_kernel(
    count, cond_hbm, nodata_hbm, gmask_hbm, gval_hbm, smask_hbm, scur_hbm, t_hbm, focal_hbm,
    r0_ref, q_ref, w_ref, z_ref, y_ref, coef_ref,
    cond_ref, nodata_ref, gmask_ref, gval_ref, smask_ref, scur_ref, focal_ref, t_ref,
    thl_ref, wts_ref, qhalo_ref, zhalo_ref, msg_ref, got_ref, zmsg_ref, zgot_ref, acc_ref, stat_ref, all_ref,
    send1, recv1, send2, recv2, send3, recv3, sem_in, sem_t,
):
    rows, cols = cond_ref.shape
    tiles = cols // LANES
    pairs = focal_ref.shape[1]
    ext = pairs + EXTRA
    groups = ext // 8
    me = lax.axis_index("space")
    last = count - 1

    barrier = pltpu.get_barrier_semaphore()
    for off in range(1, count):
        pl.semaphore_signal(
            barrier, inc=1, device_id={"space": lax.rem(me + off, count)},
            device_id_type=pl.DeviceIdType.MESH,
        )

    loads = [
        pltpu.make_async_copy(src, dst, sem_in.at[i])
        for i, (src, dst) in enumerate((
            (focal_hbm, focal_ref), (smask_hbm, smask_ref), (scur_hbm, scur_ref),
            (cond_hbm, cond_ref), (nodata_hbm, nodata_ref), (gmask_hbm, gmask_ref),
            (gval_hbm, gval_ref),
        ))
    ]

    def t_load(r):
        return pltpu.make_async_copy(t_hbm.at[r], t_ref.at[r], sem_t.at[r])

    for load in loads:
        load.start()
    for r in (0, rows - 1, *range(1, rows - 1)):
        t_load(r).start()
    for load in loads:
        load.wait()

    valid = (1 - nodata_ref[...]).astype(F32)
    active = cond_ref[...] * valid
    grounded = gmask_ref[...].astype(F32) * gval_ref[...]
    background = smask_ref[...].astype(F32) * scur_ref[...]

    def set_weights(up_a, up_v, down_a, down_v):
        lane = lax.broadcasted_iota(jnp.int32, (rows, cols), 1)
        zero = jnp.zeros((rows, cols), F32)
        row = lax.broadcasted_iota(jnp.int32, (rows, cols), 0)

        def edge(a, v):
            return 0.5 * (active + a) * valid * v

        def west(x):
            return jnp.where(lane == 0, zero, pltpu.roll(x, 1, 1))

        def east(x):
            return jnp.where(lane == cols - 1, zero, pltpu.roll(x, cols - 1, 1))

        def north(x, h):
            return jnp.where(row == 0, jnp.broadcast_to(h, x.shape), pltpu.roll(x, 1, 0))

        def south(x, h):
            return jnp.where(row == rows - 1, jnp.broadcast_to(h, x.shape), pltpu.roll(x, rows - 1, 0))

        nw = edge(north(active, up_a), north(valid, up_v))
        sw = edge(south(active, down_a), south(valid, down_v))
        ww = edge(west(active), west(valid))
        ew = edge(east(active), east(valid))
        dg = valid * (LEAKAGE + grounded) + (1.0 - valid) + nw + sw + ww + ew
        for r in range(rows):
            for i, x in enumerate((dg, nw, sw, ww, ew)):
                wts_ref[r, i:i + 1, :] = x[r:r + 1, :]

    acc_ref[...] = jnp.zeros(acc_ref.shape, F32)
    diagonal = lax.broadcasted_iota(jnp.int32, (ext, pairs), 0) == lax.broadcasted_iota(
        jnp.int32, (ext, pairs), 1)
    is_pair = lax.broadcasted_iota(jnp.int32, (ext, 1), 0) < pairs

    def column(i):
        line = jnp.broadcast_to(focal_ref[i:i + 1, :].astype(F32), (ext, pairs))
        at = jnp.sum(jnp.where(diagonal, line, 0.0), 1, keepdims=True).astype(jnp.int32)
        return jnp.where(is_pair, at, -1)

    fa, fb = column(0), column(1)

    def right_side(r):
        ids = (me * rows + r) * cols + lax.broadcasted_iota(jnp.int32, (ext, cols), 1)
        onehot = (ids == fa).astype(F32) - (ids == fb).astype(F32)
        r0_ref[r] = background[r:r + 1, :] + FOCAL_CURRENT * onehot

    right_side(0)
    right_side(rows - 1)

    def precond_row(src, dst, r, split):
        for c in range(tiles):
            cut = slice(c * LANES, (c + 1) * LANES)
            if split:
                t = t_ref[r, c]
                thi = t.astype(BF16)
                thl_ref[r, c, :, :LANES] = thi
                thl_ref[r, c, :, LANES:] = (t - thi.astype(F32)).astype(BF16)
            x = src[r, :, cut]
            hi = x.astype(BF16).astype(F32)
            lhs = jnp.concatenate([hi, x - hi], 0).astype(BF16)
            o = jnp.dot(lhs, thl_ref[r, c], preferred_element_type=F32)
            dst[r, :, cut] = o[:ext, :LANES] + (o[:ext, LANES:] + (o[ext:, :LANES] + o[ext:, LANES:]))

    def precond_inner(src, dst, split):
        def body(r, carry):
            if split:
                t_load(r).wait()
            precond_row(src, dst, r, split)
            return carry
        lax.fori_loop(1, rows - 1, body, 0)

    def stencil_group(src, dst, r, no_ref, no_i, so_ref, so_i, left, base):
        def body(g, carry):
            s = pl.ds(pl.multiple_of(g * 8, 8), 8)
            ce = src[r, s, :]
            out = (
                wts_ref[r, 0:1, :] * ce
                - wts_ref[r, 1:2, :] * no_ref[no_i, s, :]
                - wts_ref[r, 2:3, :] * so_ref[so_i, s, :]
                - wts_ref[r, 3:4, :] * pltpu.roll(ce, 1, 1)
                - wts_ref[r, 4:5, :] * pltpu.roll(ce, cols - 1, 1)
            )
            dst[r, s, :] = out
            acc_ref[base, s, :] += fold(left[r, s, :] * ce)
            acc_ref[base + 1, s, :] += fold(ce * out)
            return carry
        lax.fori_loop(0, groups, body, 0, unroll=3 if groups % 3 == 0 else 1)

    def stencil_inner(src, dst, left, base):
        def body(r, carry):
            stencil_group(src, dst, r, src, r - 1, src, r + 1, left, base)
            return carry
        lax.fori_loop(1, rows - 1, body, 0)

    def stencil_ends(src, dst, halo, left, base):
        stencil_group(src, dst, 0, halo, 0, src, 1, left, base)
        stencil_group(src, dst, rows - 1, src, rows - 2, halo, 1, left, base)

    def side_copy(src, dst, ssem, rsem, side):
        return pltpu.make_async_remote_copy(
            src_ref=src.at[side], dst_ref=dst.at[1 - side],
            send_sem=ssem.at[side], recv_sem=rsem.at[1 - side],
            device_id={"space": me - 1 if side == 0 else me + 1},
            device_id_type=pl.DeviceIdType.MESH,
        )

    has = (me > 0, me < last)

    for r in (0, rows - 1):
        t_load(r).wait()
        precond_row(r0_ref, q_ref, r, True)

    tile_a = lax.shift_right_logical(fa[:pairs] & (cols - 1), 7)
    tile_b = lax.shift_right_logical(fb[:pairs] & (cols - 1), 7)
    def pack(src, r, dst, side):
        va = src[r, :pairs, 0:LANES]
        vb = va
        for c in range(1, tiles):
            x = src[r, :pairs, c * LANES:(c + 1) * LANES]
            va = jnp.where(tile_a == c, x, va)
            vb = jnp.where(tile_b == c, x, vb)
        dst[side, 0:pairs, :] = va
        dst[side, pairs:2 * pairs, :] = vb
        for c in range(tiles):
            at = 2 * pairs + c
            dst[side, at:at + 1, :] = src[r, pairs:pairs + 1, c * LANES:(c + 1) * LANES]

    for side, r in ((0, 0), (1, rows - 1)):
        pack(q_ref, r, msg_ref, side)
        for c in range(tiles):
            cut = slice(c * LANES, (c + 1) * LANES)
            at = 2 * pairs + c
            msg_ref[side, at + tiles:at + tiles + 1, :] = active[r:r + 1, cut]
            msg_ref[side, at + 2 * tiles:at + 2 * tiles + 1, :] = valid[r:r + 1, cut]
            msg_ref[side, at + 3 * tiles:at + 3 * tiles + 1, :] = t_ref[r, c, 0:1, :]
            msg_ref[side, at + 4 * tiles:at + 4 * tiles + 1, :] = t_ref[r, c, LANES - 1:LANES, :]

    pl.semaphore_wait(barrier, last)
    for side in range(2):
        @pl.when(has[side])
        def _():
            side_copy(msg_ref, got_ref, send1, recv1, side).start()

        @pl.when(jnp.logical_not(has[side]))
        def _():
            got_ref[side] = jnp.zeros(got_ref.shape[1:], F32)
            zgot_ref[side] = jnp.zeros(zgot_ref.shape[1:], F32)

    zhalo_ref[...] = jnp.zeros(zhalo_ref.shape, F32)
    none = jnp.zeros((1, cols), F32)
    set_weights(none, none, none, none)
    for r in range(1, rows - 1):
        right_side(r)
    precond_inner(r0_ref, q_ref, True)
    stencil_inner(q_ref, w_ref, r0_ref, 0)

    def done(src, dst, ssem, rsem):
        for side in range(2):
            @pl.when(has[side])
            def _():
                side_copy(src, dst, ssem, rsem, side).wait_send()
                pltpu.make_async_remote_copy(
                    src_ref=src.at[1 - side], dst_ref=dst.at[side],
                    send_sem=ssem.at[1 - side], recv_sem=rsem.at[side],
                    device_id={"space": me - 1 if side == 0 else me + 1},
                    device_id_type=pl.DeviceIdType.MESH,
                ).wait_recv()

    done(msg_ref, got_ref, send1, recv1)

    def row_of(side, base):
        return jnp.concatenate([got_ref[side, base + c:base + c + 1, :] for c in range(tiles)], 1)

    a_at, v_at = 2 * pairs + tiles, 2 * pairs + 2 * tiles
    set_weights(row_of(0, a_at), row_of(0, v_at), row_of(1, a_at), row_of(1, v_at))
    for side in range(2):
        va = got_ref[side, 0:pairs, :]
        vb = got_ref[side, pairs:2 * pairs, :]
        for c in range(tiles):
            cut = slice(c * LANES, (c + 1) * LANES)
            common = got_ref[side, 2 * pairs + c:2 * pairs + c + 1, :]
            qhalo_ref[side, 0:pairs, cut] = jnp.where(
                tile_a == c, va, jnp.where(tile_b == c, vb, jnp.broadcast_to(common, va.shape))
            )
            qhalo_ref[side, pairs:ext, cut] = jnp.broadcast_to(common, (EXTRA, LANES))

    stencil_ends(q_ref, w_ref, qhalo_ref, r0_ref, 0)
    precond_row(w_ref, z_ref, 0, False)
    precond_row(w_ref, z_ref, rows - 1, False)

    ends_at = 2 * pairs + tiles
    lane_e = lax.broadcasted_iota(jnp.int32, (pairs, LANES), 1)
    for side, r in ((0, 0), (1, rows - 1)):
        pack(z_ref, r, zmsg_ref, side)
        ends = jnp.zeros((pairs, LANES), F32)
        for c in range(tiles):
            cut = slice(c * LANES, (c + 1) * LANES)
            diff = w_ref[r, :pairs, cut] - w_ref[r, pairs:pairs + 1, cut]
            ends = jnp.where(lane_e == c, jnp.broadcast_to(diff[:, 0:1], ends.shape), ends)
            ends = jnp.where(lane_e == tiles + c, jnp.broadcast_to(diff[:, LANES - 1:], ends.shape), ends)
        zmsg_ref[side, ends_at:ends_at + pairs, :] = ends

    for side in range(2):
        @pl.when(has[side])
        def _():
            side_copy(zmsg_ref, zgot_ref, send2, recv2, side).start()

    precond_inner(w_ref, z_ref, False)
    stencil_inner(z_ref, y_ref, w_ref, 2)
    stencil_ends(z_ref, y_ref, zhalo_ref, w_ref, 2)

    done(zmsg_ref, zgot_ref, send2, recv2)
    cross = jnp.zeros((pairs, LANES), F32)
    for side in range(2):
        va = zgot_ref[side, 0:pairs, :]
        vb = zgot_ref[side, pairs:2 * pairs, :]
        ends = zgot_ref[side, ends_at:ends_at + pairs, :]
        for c in range(tiles):
            cut = slice(c * LANES, (c + 1) * LANES)
            common = zgot_ref[side, 2 * pairs + c:2 * pairs + c + 1, :]
            at = 2 * pairs + 3 * tiles + c
            other = (
                common
                + ends[:, c:c + 1] * got_ref[side, at:at + 1, :]
                + ends[:, tiles + c:tiles + c + 1] * got_ref[side, at + tiles:at + tiles + 1, :]
            )
            halo = jnp.where(tile_a == c, va, jnp.where(tile_b == c, vb, other))
            r, kind = ((0, 1), (rows - 1, 2))[side]
            term = wts_ref[r, kind:kind + 1, cut] * halo
            y_ref[r, :pairs, cut] -= term
            cross = cross - z_ref[r, :pairs, cut] * term
    acc_ref[3, :pairs, :] += cross

    lane = lax.broadcasted_iota(jnp.int32, (LANES, LANES), 1)
    table = jnp.zeros((LANES, LANES), F32)
    pad = jnp.zeros((LANES - pairs, 1), F32)
    for i in range(4):
        col = jnp.concatenate([jnp.sum(acc_ref[i, :pairs, :], 1, keepdims=True), pad], 0)
        table = jnp.where(lane == i, jnp.broadcast_to(col, table.shape), table)
    mine = table.T[0:8, :]
    stat_ref[...] = mine

    def stat_copy(slot, peer, k):
        return pltpu.make_async_remote_copy(
            src_ref=stat_ref, dst_ref=all_ref.at[slot],
            send_sem=send3.at[k], recv_sem=recv3.at[k],
            device_id={"space": peer}, device_id_type=pl.DeviceIdType.MESH,
        )

    for k in range(1, count):
        stat_copy(k - 1, lax.rem(me + k, count), k - 1).start()
    for k in range(1, count):
        stat_copy(k - 1, lax.rem(me + k, count), k - 1).wait()
    total = mine
    for k in range(1, count):
        total = total + all_ref[k - 1]
    back = jnp.concatenate([total, jnp.zeros((LANES - 8, LANES), F32)], 0).T
    gamma0, kappa, mu, nu = (back[:pairs, i:i + 1] for i in range(4))
    a0 = gamma0 / kappa
    gamma1 = a0 * a0 * mu - gamma0
    beta = gamma1 / gamma0
    a1 = gamma1 / (kappa - 2.0 * a0 * mu + a0 * a0 * nu - beta * gamma1 / a0)
    first = a0 + a1 * (1.0 + beta)
    lane_p = lax.broadcasted_iota(jnp.int32, (pairs, LANES), 1)
    coef_ref[...] = jnp.where(lane_p < LANES // 2, first, a0 * a1)


def combine_kernel(coef_ref, r0_ref, q_ref, w_ref, z_ref, y_ref, sol_hbm, res_hbm, sol_ref, res_ref, sem):
    pairs, rows, cols = sol_ref.shape
    block = 8

    def out(i, src, dst, k):
        cut = pl.ds(pl.multiple_of(i * block, block), block)
        return pltpu.make_async_copy(src.at[cut], dst.at[cut], sem.at[k, i])

    def body(i, carry):
        cut = pl.ds(pl.multiple_of(i * block, block), block)
        one = coef_ref[cut, 0:1]
        two = coef_ref[cut, LANES - 1:LANES]
        for r in range(rows):
            sol_ref[cut, r, :] = one * q_ref[r, cut, :] - two * z_ref[r, cut, :]
            res_ref[cut, r, :] = r0_ref[r, cut, :] - one * w_ref[r, cut, :] + two * y_ref[r, cut, :]
        out(i, sol_ref, sol_hbm, 0).start()
        out(i, res_ref, res_hbm, 1).start()
        return carry

    lax.fori_loop(0, pairs // block, body, 0)

    def finish(i, carry):
        out(i, sol_ref, sol_hbm, 0).wait()
        out(i, res_ref, res_hbm, 1).wait()
        return carry

    lax.fori_loop(0, pairs // block, finish, 0)


def on_device(count, cond, nodata, gmask, gval, smask, scur, tinv, focal):
    rows, cols = cond.shape
    pairs = focal.shape[0]
    tiles = cols // LANES
    ext = pairs + EXTRA
    field = jax.ShapeDtypeStruct((rows, ext, cols), F32)
    vm = pl.BlockSpec(memory_space=pltpu.VMEM)
    hbm = pl.BlockSpec(memory_space=pltpu.HBM)
    msg = (2, 2 * pairs + 5 * tiles, LANES)
    zmsg = (2, 3 * pairs + tiles, LANES)
    others = count - 1
    small = (rows, cols)
    r0, q, w, z, y, coef = pl.pallas_call(
        functools.partial(krylov_kernel, count),
        out_shape=[field] * 5 + [jax.ShapeDtypeStruct((pairs, LANES), F32)],
        in_specs=[hbm] * 8,
        out_specs=[vm] * 6,
        scratch_shapes=[
            pltpu.VMEM(small, F32),
            pltpu.VMEM(small, jnp.int32),
            pltpu.VMEM(small, jnp.int32),
            pltpu.VMEM(small, F32),
            pltpu.VMEM(small, jnp.int32),
            pltpu.VMEM(small, F32),
            pltpu.VMEM((2, pairs), jnp.int32),
            pltpu.VMEM(tinv.shape, F32),
            pltpu.VMEM((rows, tiles, LANES, 2 * LANES), BF16),
            pltpu.VMEM((rows, 8, cols), F32),
            pltpu.VMEM((2, ext, cols), F32),
            pltpu.VMEM((2, ext, cols), F32),
            pltpu.VMEM(msg, F32),
            pltpu.VMEM(msg, F32),
            pltpu.VMEM(zmsg, F32),
            pltpu.VMEM(zmsg, F32),
            pltpu.VMEM((4, ext, LANES), F32),
            pltpu.VMEM((8, LANES), F32),
            pltpu.VMEM((others, 8, LANES), F32),
            pltpu.SemaphoreType.DMA((2,)),
            pltpu.SemaphoreType.DMA((2,)),
            pltpu.SemaphoreType.DMA((2,)),
            pltpu.SemaphoreType.DMA((2,)),
            pltpu.SemaphoreType.DMA((others,)),
            pltpu.SemaphoreType.DMA((others,)),
            pltpu.SemaphoreType.DMA((7,)),
            pltpu.SemaphoreType.DMA((rows,)),
        ],
        compiler_params=pltpu.CompilerParams(
            collective_id=0, has_side_effects=True, vmem_limit_bytes=36 * 1024 * 1024
        ),
        name="krylov",
    )(*(
        pltpu.with_memory_space_constraint(x, pltpu.HBM)
        for x in (cond, nodata, gmask, gval, smask, scur, tinv, focal.T)
    ))

    out = jax.ShapeDtypeStruct((pairs, rows, cols), F32)
    return tuple(pl.pallas_call(
        combine_kernel,
        out_shape=[out, out],
        in_specs=[vm] * 6,
        out_specs=[hbm, hbm],
        scratch_shapes=[
            pltpu.VMEM(out.shape, F32),
            pltpu.VMEM(out.shape, F32),
            pltpu.SemaphoreType.DMA((2, pairs // 8)),
        ],
        compiler_params=pltpu.CompilerParams(vmem_limit_bytes=20 * 1024 * 1024),
        name="combine",
    )(coef, r0, q, w, z, y))


def solution(mesh):
    return jax.shard_map(
        functools.partial(on_device, mesh.shape["space"]),
        mesh=mesh,
        in_specs=(
            P(("groups", "space"), None),
            P(("groups", "space"), None),
            P(("groups", "space"), None),
            P(("groups", "space"), None),
            P(("groups", "space"), None),
            P(("groups", "space"), None),
            P(("groups", "space"), None, None, None),
            P(("groups", "rhs"), None),
        ),
        out_specs=(P("rhs", ("groups", "space"), None), P("rhs", ("groups", "space"), None)),
        check_vma=False,
    )
```
